128 devices in a mesh: row: 8 (over x_hi, z), col: 16 (over x_lo, y, core).
Axes of the slice: x: 4 (x_hi: 2, x_lo: 2; x = x_hi * 2 + x_lo), y: 4, z: 4, core: 2. Of those that a mesh axis runs over, the one named last changes fastest.
Arguments:
- tokens: bfloat16 [1024, 12288], P('row', 'col'), may hold values from -6 to 6
- prev_tokens: bfloat16 [1024, 12288], P('row', 'col'), may hold values from -6 to 6
- hidden_grad: bfloat16 [1024, 49152], P('col', 'row'), may hold values from -6 to 6
- active_blocks: int32 [1], replicated, may hold values from 6 to 16
- weight: bfloat16 [12288, 49152], P('col', 'row'), may hold values from -0.0546875 to 0.0546875
Outputs:
- activation: bfloat16 [1024, 49152], P('col', 'row')
- weight_grad: bfloat16 [12288, 49152], P('col', 'row')
The draws below stay inside these ranges and needn't reach their ends.
Inputs may be any that keep to these rules, and one draw needn't show every extreme that they name: The sampled blocks are the first active_blocks[0] blocks of 3072 hidden units.
All inputs are finite; a program needn't handle non-finite values.
Results may differ from the reference program's by a relative error of at most 0.001.
Values may be sent and summed in bfloat16 or wider, within the bound.
No kernel may reach another device: no remote copies, remote signals or barrier semaphores. Data moves between devices by JAX's collectives and lax.ppermute only.
A program may use at most 640 MiB of HBM per device.

```python
import jax
import jax.numpy as jnp
from jax import lax

D = 12288
FF = 49152
BLOCK = 3072
TOKENS = 1024
DSLAB = 768
N_COL = 16


def shard_levels(stream_key, extent, shards, least, largest):
    def one(dim, blocks):
        steps = jax.random.uniform(jax.random.fold_in(jax.random.fold_in(stream_key, 6), dim), (blocks,), jnp.float32, least / len(shards), largest / len(shards))
        return jnp.repeat(jnp.exp(steps), extent[dim] // blocks).reshape((-1,) + (1,) * (len(extent) - dim - 1))

    loudness = one(*shards[0])
    for cut in shards[1:]:
        loudness = loudness * one(*cut)
    return loudness


def gaussian(own_key, extent, spread, bound, pieces=(), held_as=jnp.bfloat16):
    array = jax.random.normal(own_key, extent, jnp.float32) * spread
    if len(pieces) > 0:
        array = shard_levels(own_key, extent, pieces, -0.22, 0.18) * array
    return jnp.clip(array, min=-bound, max=bound).astype(held_as)


def setup_inputs(seed: int = 0) -> dict:
    seeds = jax.random.split(jax.random.key(seed), 6)
    return {
        "tokens": gaussian(seeds[0], (TOKENS, D), 1.0, 6.0, ((0, 8), (1, 16))),
        "prev_tokens": gaussian(seeds[1], (TOKENS, D), 1.0, 6.0, ((0, 8), (1, 16))),
        "hidden_grad": gaussian(seeds[2], (TOKENS, FF), 1.0, 6.0, ((0, 16), (1, 8))),
        "active_blocks": jax.random.randint(seeds[3], (1,), 6, 17).astype(jnp.int32),
        "weight": gaussian(seeds[4], (D, FF), D ** -0.5, 0.0546875, ((0, 16), (1, 8))),
    }


def reference(tokens, prev_tokens, hidden_grad, active_blocks, weight):
    unit_limit = active_blocks[0] * BLOCK
    unit_mask = (jnp.arange(FF, dtype=jnp.int32) < unit_limit).astype(jnp.float32)

    def add_slab(running, index):
        columns = lax.dynamic_slice_in_dim(tokens, (index * DSLAB).astype(jnp.int32), DSLAB, 1)
        weight_rows = lax.dynamic_slice_in_dim(weight, (index * DSLAB).astype(jnp.int32), DSLAB, 0)
        partial_value = jnp.dot(columns, weight_rows, preferred_element_type=jnp.float32)
        return running + partial_value, None

    hidden, unused = lax.scan(add_slab, jnp.zeros((TOKENS, FF), jnp.float32), jnp.arange(N_COL, dtype=jnp.int32))
    activation = (jax.nn.gelu(hidden, approximate=False) * unit_mask).astype(jnp.bfloat16)

    def grad_block(index):
        offset = (index * BLOCK).astype(jnp.int32)
        grad_cols = lax.dynamic_slice_in_dim(hidden_grad, offset, BLOCK, 1)
        mask_cols = lax.dynamic_slice_in_dim(unit_mask, offset, BLOCK, 0)
        block_grad = lax.dot_general(prev_tokens, grad_cols, (((0,), (0,)), ((), ())), preferred_element_type=jnp.float32)
        return (block_grad * mask_cols).astype(jnp.bfloat16)

    blocks = lax.map(grad_block, jnp.arange(FF // BLOCK, dtype=jnp.int32))
    weight_grad = jnp.transpose(blocks, (1, 0, 2)).reshape(D, FF)
    return activation, weight_grad
```

```python
import jax
import jax.numpy as jnp
from jax import lax
from jax.experimental import pallas as pl
from jax.experimental.pallas import tpu as pltpu
from jax.sharding import PartitionSpec as P

BLOCK = 3072
F32, BF16, I16, I32 = jnp.float32, jnp.bfloat16, jnp.int16, jnp.int32


def perm(f):
    out = []
    for i in range(128):
        r, c = divmod(i, 16)
        xh, z, xl, y, k = f(r // 4, r % 4, c // 8, (c // 2) % 4, c % 2)
        out.append((i, (xh * 4 + z % 4) * 16 + xl * 8 + (y % 4) * 2 + k))
    return out


SIB = perm(lambda h, z, x, y, k: (h, z, x, y, 1 - k))
XLO = perm(lambda h, z, x, y, k: (h, z, 1 - x, y, k))
XHI = perm(lambda h, z, x, y, k: (1 - h, z, x, y, k))
YUP = perm(lambda h, z, x, y, k: (h, z, x, y + 1, k))
YDN = perm(lambda h, z, x, y, k: (h, z, x, y - 1, k))
YTWO = perm(lambda h, z, x, y, k: (h, z, x, y + 2, k))
ZUP = perm(lambda h, z, x, y, k: (h, z + 1, x, y, k))
ZDN = perm(lambda h, z, x, y, k: (h, z - 1, x, y, k))
ZTWO = perm(lambda h, z, x, y, k: (h, z + 2, x, y, k))


def send(a, p):
    return lax.ppermute(a, ("row", "col"), p)


OFFS = (0, -1, 1, 2)
LANES = 128


def encode(v, ref, rows=None):
    n = v.shape[1]
    top = jnp.maximum(jnp.max(jnp.abs(v), axis=1, keepdims=True), 2.0 ** -100)
    e = jnp.floor(jnp.log2(top * (1 + 2.0 ** -10))) + 1
    mant = jnp.ceil(top * jnp.exp2(15 - e))
    scale = mant * jnp.exp2(e - 15) * (1 / 32767)
    q = jnp.round(v * (1 / scale)).astype(I32).astype(I16)
    lane = lax.broadcasted_iota(I32, (v.shape[0], LANES), 1)
    tag = jnp.where(lane < 64, mant, e).astype(I32).astype(I16)
    if rows is None:
        ref[:, :n] = q
        ref[:, n:] = tag
    else:
        ref[rows, :n] = q
        ref[rows, n:] = tag


def decode(ref, rows, cols=None):
    n = ref.shape[1] - LANES
    tag = ref[rows, n:].astype(I32).astype(F32)
    scale = tag[:, 0:1] * jnp.exp2(tag[:, 64:65] - 15) * (1 / 32767)
    q = ref[rows, :n] if cols is None else ref[rows, cols]
    return q.astype(I32).astype(F32) * scale


def first_kernel(ids, *refs):
    ts, (w_own, w_sib), (m_up, m_dn, t_out), (t_std, t_rel, acc) = refs[:8], refs[8:10], refs[10:13], refs[13:]
    i = pl.program_id(0)
    tn = w_own.shape[1]
    slab = w_own.shape[0]
    y, xl, z, xh = ids[1], ids[2], ids[3], ids[4]

    @pl.when(i == 0)
    def _():
        for half in range(2):
            for j, off in enumerate(OFFS):
                for s in range(2):
                    at = lax.rem(z + off + 4, 4) * 2 + lax.rem(xh + s, 2)
                    t_std[at, :, half * slab:(half + 1) * slab] = ts[half * 4 + j][s]
        for s in range(2):
            t_rel[s * 128:(s + 1) * 128] = t_std[lax.rem(y + 2, 4) * 2 + lax.rem(xl + 1 + s, 2)]
            for j, off in enumerate((1, -1, 0)):
                at = lax.rem(y + off + 4, 4) * 2 + lax.rem(xl + 1 + s, 2)
                t_out[(2 * j + s) * 128:(2 * j + s + 1) * 128] = t_std[at]

    part = jnp.dot(t_rel[:, :slab], w_own[...], preferred_element_type=F32)
    part += jnp.dot(t_rel[:, slab:], w_sib[...], preferred_element_type=F32)
    acc[:, pl.ds(pl.multiple_of(i * tn, tn), tn)] = part

    @pl.when(i == pl.num_programs(0) - 1)
    def _():
        h = acc.shape[1] // 2
        for r in range(0, acc.shape[0], 32):
            rows = slice(r, r + 32)
            encode(acc[rows, :h], m_up, rows)
            encode(acc[rows, h:], m_dn, rows)


def second_kernel(ids, t, w_own, w_sib, m_up, m_dn, r_up, r_dn, s_own, acc):
    i = pl.program_id(0)
    tn = w_own.shape[1]
    slab = w_own.shape[0]
    part = jnp.dot(t[:, :slab], w_own[...], preferred_element_type=F32)
    part += jnp.dot(t[:, slab:], w_sib[...], preferred_element_type=F32)
    acc[:, pl.ds(pl.multiple_of(i * tn, tn), tn)] = part

    @pl.when(i == pl.num_programs(0) - 1)
    def _():
        h = acc.shape[1] // 2
        for r in range(0, 256, 32):
            rows = slice(r, r + 32)
            encode(acc[r:r + 32, h:], m_up, rows)
            encode(acc[256 + r:288 + r, :h], m_dn, rows)
        r_up[...] = acc[:256, :h]
        r_dn[...] = acc[256:512, h:]
        s_own[...] = acc[512:]


def relay_kernel(m, r, first, second):
    half = r.shape[0] // 2
    for at in range(0, 2 * half, 32):
        rows = slice(at, at + 32)
        v = r[rows, :] + decode(m, rows)
        if at < half:
            encode(v, first, rows)
        else:
            encode(v, second, slice(at - half, at - half + 32))


def fold(s, m2_up, m2_dn, m3_up, m3_dn, at, base):
    h = s.shape[1] // 2
    rows, mine = slice(base + at, base + at + 32), slice(at, at + 32)
    left = s[rows, :h] + (decode(m3_up, mine) + decode(m2_dn, rows))
    right = s[rows, h:] + (decode(m2_up, rows) + decode(m3_dn, mine))
    return jnp.concatenate([left, right], axis=1)


def give_kernel(s, m2_up, m2_dn, m3_up, m3_dn, out):
    for at in range(0, 128, 32):
        encode(fold(s, m2_up, m2_dn, m3_up, m3_dn, at, 0), out, slice(at, at + 32))


def keep_kernel(s, m2_up, m2_dn, m3_up, m3_dn, x, out):
    for at in range(0, 128, 32):
        out[at:at + 32, :] = fold(s, m2_up, m2_dn, m3_up, m3_dn, at, 128) + decode(x, slice(at, at + 32))


def earlier_kernel(ids, p0, p1, p2, p3, out, std):
    core, y, xl, z, xh = ids[0], ids[1], ids[2], ids[3], ids[4]
    for j, off in enumerate(OFFS):
        for s in range(2):
            at = lax.rem(z + off + 4, 4) * 2 + lax.rem(xh + s, 2)
            std[pl.ds(pl.multiple_of(at * 128, 128), 128), :] = (p0, p1, p2, p3)[j][s]
    for s in range(2):
        for j, off in enumerate(OFFS):
            at = (lax.rem(y + off + 4, 4) + lax.rem(xl + s, 2) * 0) * 2 + lax.rem(xl + s, 2)
            own = std[pl.ds(pl.multiple_of(at * 128 + core * 64, 64), 64), :]
            sib = std[pl.ds(pl.multiple_of(at * 128 + (1 - core) * 64, 64), 64), :]
            i = s * 4 + j
            out[:, i * 128:(i + 1) * 128] = jnp.concatenate([own, sib], axis=0).T


def grad_kernel(ids, *refs):
    own, sib, p_t, out, rhs = refs[:8], refs[8:16], refs[16], refs[17], refs[18]
    for j in range(8):
        rhs[j * 128:j * 128 + 64, :] = own[j][...]
        rhs[j * 128 + 64:j * 128 + 128, :] = sib[j][...]
    tn = out.shape[1]
    unit = ids[5] + pl.program_id(0) * tn + lax.broadcasted_iota(I32, (1, tn), 1)
    mask = (unit < ids[6]).astype(F32)
    grad = jnp.dot(p_t[...], rhs[...], preferred_element_type=F32)
    out[...] = (grad * mask).astype(BF16)


def vmem():
    return pl.BlockSpec(memory_space=pltpu.VMEM)


def shards(tokens, prev_tokens, hidden_grad, active_blocks, weight):
    slab, units = weight.shape
    half = units // 2
    row, col = lax.axis_index("row"), lax.axis_index("col")
    core = col % 2
    ids = jnp.stack([core, (col // 2) % 4, col // 8, row % 4, row // 4, row * units, active_blocks[0] * BLOCK, 0]).astype(I32)
    params = pltpu.CompilerParams(vmem_limit_bytes=56 << 20)

    def call(f, outs, grid=None, specs=None, out_specs=None, scratch=(), with_ids=True, flops=0):
        kw = dict(out_shape=outs, compiler_params=params)
        if flops:
            kw["cost_estimate"] = pl.CostEstimate(flops=flops, bytes_accessed=16 << 20, transcendentals=0)
        if with_ids:
            spec = pltpu.PrefetchScalarGridSpec(num_scalar_prefetch=1, grid=grid or (), in_specs=specs, out_specs=out_specs, scratch_shapes=scratch)
            return pl.pallas_call(f, grid_spec=spec, **kw)
        return pl.pallas_call(f, in_specs=specs, out_specs=out_specs, scratch_shapes=scratch, **kw)

    def gather_row(a):
        near = jnp.stack([a, send(a, XHI)])
        return [near, send(near, ZUP), send(near, ZDN), send(near, ZTWO)]

    t_own = gather_row(tokens)
    t_sib = [send(a, SIB) for a in t_own]
    w_sib = send(lax.dynamic_slice(weight, (0, (1 - core) * half), (slab, half)), SIB)

    h_own = [hidden_grad, send(hidden_grad, YUP), send(hidden_grad, YDN), send(hidden_grad, YTWO)]
    h_own = h_own + [send(a, XLO) for a in h_own]
    h_sib = [send(a, SIB) for a in h_own]

    p_own = gather_row(prev_tokens)

    tn = 512
    nt = half // tn
    msg = (256, half // 2 + LANES)
    w_specs = [pl.BlockSpec((slab, tn), lambda i, s: (0, s[0] * nt + i)), pl.BlockSpec((slab, tn), lambda i, s: (0, i))]
    whole = lambda shape: pl.BlockSpec(shape, lambda i, s: (0,) * len(shape))
    m1_up, m1_dn, t_rest = call(
        first_kernel,
        [jax.ShapeDtypeStruct(msg, I16), jax.ShapeDtypeStruct(msg, I16), jax.ShapeDtypeStruct((768, 2 * slab), BF16)],
        (nt,), [whole((2, 128, slab))] * 8 + w_specs, [whole(msg), whole(msg), whole((768, 2 * slab))],
        [pltpu.VMEM((8, 128, 2 * slab), BF16), pltpu.VMEM((256, 2 * slab), BF16), pltpu.VMEM((256, half), F32)],
        flops=2 * 256 * 2 * slab * half,
    )(ids, *t_own, *t_sib, weight, w_sib)
    m1_up, m1_dn = send(m1_up, YUP), send(m1_dn, YDN)
    rest = (256, half // 2)
    m2_up, m2_dn, r_up, r_dn, s_own = call(
        second_kernel,
        [jax.ShapeDtypeStruct(msg, I16), jax.ShapeDtypeStruct(msg, I16), jax.ShapeDtypeStruct(rest, F32), jax.ShapeDtypeStruct(rest, F32), jax.ShapeDtypeStruct((256, half), F32)],
        (nt,), [whole((768, 2 * slab))] + w_specs, [whole(msg), whole(msg), whole(rest), whole(rest), whole((256, half))],
        [pltpu.VMEM((768, half), F32)],
        flops=2 * 768 * 2 * slab * half,
    )(ids, t_rest, weight, w_sib)
    m2_up, m2_dn = send(m2_up, YUP), send(m2_dn, YDN)

    piece = jax.ShapeDtypeStruct((128, half // 2 + LANES), I16)
    relay = call(relay_kernel, [piece, piece], specs=[vmem()] * 2, out_specs=[vmem()] * 2, with_ids=False, flops=1 << 20)
    up1, up2 = relay(m1_up, r_up)
    dn1, dn2 = relay(m1_dn, r_dn)
    up1, dn1 = send(up1, YUP), send(dn1, YDN)
    up2, dn2 = send(up2, YUP), send(dn2, YDN)
    x_msg = jax.ShapeDtypeStruct((128, half + LANES), I16)
    give = call(give_kernel, x_msg, specs=[vmem()] * 5, out_specs=vmem(), with_ids=False, flops=1 << 20)
    x_in = send(give(s_own, m2_up, m2_dn, up1, dn1), XLO)
    keep = call(keep_kernel, jax.ShapeDtypeStruct((128, half), F32), specs=[vmem()] * 6, out_specs=vmem(), with_ids=False, flops=1 << 20)
    hidden = keep(s_own, m2_up, m2_dn, up2, dn2, x_in)

    unit_ids = row * units + core * half + lax.iota(I32, half)
    unit_mask = (unit_ids < active_blocks[0] * BLOCK).astype(F32)
    act = (jax.nn.gelu(hidden, approximate=False) * unit_mask).astype(BF16)
    act_own = lax.dynamic_slice(act, (core * 64, 0), (64, half))
    act_sib = send(lax.dynamic_slice(act, ((1 - core) * 64, 0), (64, half)), SIB)
    activation = jnp.where(core == 0, jnp.concatenate([act_own, act_sib], 1), jnp.concatenate([act_sib, act_own], 1))

    p_t = call(
        earlier_kernel, jax.ShapeDtypeStruct((slab, 1024), BF16), (), [vmem()] * 4, vmem(),
        [pltpu.VMEM((1024, slab), BF16)], flops=1 << 20,
    )(ids, *p_own)
    tg = 512
    weight_grad = call(
        grad_kernel, jax.ShapeDtypeStruct((slab, units), BF16), (units // tg,),
        [pl.BlockSpec((64, tg), lambda i, s: (0, i))] * 16 + [whole((slab, 1024))],
        pl.BlockSpec((slab, tg), lambda i, s: (0, i)), [pltpu.VMEM((1024, tg), BF16)],
        flops=2 * 1024 * slab * units,
    )(ids, *h_own, *h_sib, p_t)
    return (activation, weight_grad)


def solution(mesh):
    return jax.shard_map(
        shards,
        mesh=mesh,
        in_specs=(P("row", "col"), P("row", "col"), P("col", "row"), P(), P("col", "row")),
        out_specs=(P("col", "row"), P("col", "row")),
        check_vma=False,
    )
```

```python
from functools import partial

import jax
import jax.numpy as jnp
from jax import lax
from jax.experimental import pallas as pl
from jax.experimental.pallas import tpu as pltpu
from jax.sharding import PartitionSpec as P


BLOCK = 3072
ROUND = 1.5 * 2.0 ** 23
F32, BF16, I16, I32 = jnp.float32, jnp.bfloat16, jnp.int16, jnp.int32


def perm(f):
    out = []
    for i in range(128):
        r, c = divmod(i, 16)
        xh, z, xl, y, k = f(r // 4, r % 4, c // 8, (c // 2) % 4, c % 2)
        out.append((i, (xh * 4 + z % 4) * 16 + xl * 8 + (y % 4) * 2 + k))
    return out


SIB = perm(lambda h, z, x, y, k: (h, z, x, y, 1 - k))
XLO = perm(lambda h, z, x, y, k: (h, z, 1 - x, y, k))
XHI = perm(lambda h, z, x, y, k: (1 - h, z, x, y, k))
YUP = perm(lambda h, z, x, y, k: (h, z, x, y + 1, k))
YDN = perm(lambda h, z, x, y, k: (h, z, x, y - 1, k))
YTWO = perm(lambda h, z, x, y, k: (h, z, x, y + 2, k))
ZUP = perm(lambda h, z, x, y, k: (h, z + 1, x, y, k))
ZDN = perm(lambda h, z, x, y, k: (h, z - 1, x, y, k))
ZTWO = perm(lambda h, z, x, y, k: (h, z + 2, x, y, k))


def send(a, p):
    return lax.ppermute(a, ("row", "col"), p)


OFFS = (0, -1, 1, 2)
TAG = 16
PART_LIMIT = 24
ROOT_HALF = 0.5 ** 0.5


def encode(v, ref, cols, base=0):
    rows = v.shape[0]
    top = jnp.maximum(jnp.max(jnp.abs(v), axis=0, keepdims=True), 2.0 ** -100)
    e = jnp.floor(jnp.log2(top * (1 + 2.0 ** -10))) + 1
    mant = jnp.ceil(top * jnp.exp2(15 - e))
    scale = mant * jnp.exp2(e - 15) * (1 / 32767)
    q = v * (1 / scale) + ROUND - ROUND
    ref[base:base + rows, cols] = q.astype(I32).astype(I16)
    sub = lax.broadcasted_iota(I32, (TAG, v.shape[1]), 0)
    ref[base + rows:base + rows + TAG, cols] = jnp.where(sub < TAG // 2, mant, e).astype(I32).astype(I16)


def decode(ref, rows, cols):
    n = ref.shape[0] - TAG
    tag = ref[n:, cols].astype(I32).astype(F32)
    scale = tag[0:1] * jnp.exp2(tag[TAG // 2:TAG // 2 + 1] - 15) * (1 / 32767)
    return ref[rows, cols].astype(I32).astype(F32) * scale


def over_columns(n, width, body):
    def step(i, c):
        body(pl.multiple_of(i * width, width))
        return c

    lax.fori_loop(0, n // width, step, 0)


def load_kernel(ids, w, w_far, own, sib, sems):
    half = own.shape[1]
    cols = pl.ds(pl.multiple_of(ids[0] * half, half), half)
    copies = [pltpu.make_async_copy(src.at[:, cols], dst, sems.at[i]) for i, (src, dst) in enumerate(((w, own), (w_far, sib)))]
    for c in copies:
        c.start()
    for c in copies:
        c.wait()


def part_kernel(ids, *refs):
    n = (len(refs) - 2) // 3
    own, sib, (w_own, w_sib), outs = refs[:n], refs[n:2 * n], refs[2 * n:2 * n + 2], refs[2 * n + 2:]
    slab, half = w_own.shape
    lhs = jnp.concatenate(
        [jnp.concatenate([a[...].reshape(256, slab), b[...].reshape(256, slab)], axis=1) for a, b in zip(own, sib)], axis=0
    )

    def block(c):
        cols = pl.ds(c, 512)
        part = jnp.dot(lhs, jnp.concatenate([w_own[:, cols], w_sib[:, cols]], axis=0), preferred_element_type=F32)
        for j, out in enumerate(outs):
            out[:, cols] = part[j * 256:(j + 1) * 256]

    for c in range(0, half, 512):
        block(c)


def with_part(ids, parts, off, f):
    k = lax.rem(ids[1] - ids[3] + off + 8, 4)
    for part, j in zip(parts, (0, 3, 1, 2)):
        pl.when(k == j)(lambda part=part: f(part))


def side(ids, s):
    return pl.ds(pl.multiple_of(lax.rem(ids[2] + ids[4] + 1 + s, 2) * 128, 128), 128)


def first_kernel(ids, *refs):
    parts, (m_up, m_dn) = refs[:4], refs[4:]
    h = m_up.shape[1]

    def f(part):
        def block(c):
            cols, far = pl.ds(c, 256), pl.ds(c + h, 256)
            for out, at in ((m_up, cols), (m_dn, far)):
                encode(jnp.concatenate([part[side(ids, 0), at], part[side(ids, 1), at]], axis=0), out, cols)

        over_columns(h, 256, block)

    with_part(ids, parts, 2, f)


def second_kernel(ids, *refs):
    parts, (up1, up2, dn1, dn2) = refs[:4], refs[4:]
    h = up1.shape[1]

    def go(part, one, two, base):
        def block(c):
            encode(part[side(ids, 0), pl.ds(c + base, 256)], one, pl.ds(c, 256))
            encode(part[side(ids, 1), pl.ds(c + base, 256)], two, pl.ds(c, 256))

        over_columns(h, 256, block)

    with_part(ids, parts, 1, lambda part: go(part, up1, up2, h))
    with_part(ids, parts, -1, lambda part: go(part, dn1, dn2, 0))


def relay_kernel(off, ids, *refs):
    parts, m, first, second = refs[:4], refs[4], refs[5], refs[6]
    h = m.shape[1]
    base = 0 if off == 1 else h

    def f(part):
        def block(c):
            cols, at = pl.ds(c, 256), pl.ds(c + base, 256)
            encode(part[side(ids, 0), at] + decode(m, slice(0, 128), cols), first, cols)
            encode(part[side(ids, 1), at] + decode(m, slice(128, 256), cols), second, cols)

        over_columns(h, 256, block)

    with_part(ids, parts, off, f)


def give_kernel(ids, *refs):
    parts, (m2_up, m2_dn, m3_up, m3_dn, out) = refs[:4], refs[4:]
    h = m2_up.shape[1]
    rows = slice(0, 128)

    def f(part):
        def block(c):
            cols, far = pl.ds(c, 256), pl.ds(c + h, 256)
            encode(part[side(ids, 0), cols] + (decode(m3_up, rows, cols) + decode(m2_dn, rows, cols)), out, cols)
            encode(part[side(ids, 0), far] + (decode(m2_up, rows, cols) + decode(m3_dn, rows, cols)), out, far)

        over_columns(h, 256, block)

    with_part(ids, parts, 0, f)


def keep_kernel(ids, *refs):
    parts, (m2_up, m2_dn, m3_up, m3_dn, x, own, sib) = refs[:4], refs[4:]
    h = m2_up.shape[1]
    core = ids[0]
    start = lax.rem(ids[2] + ids[4], 2) * 128

    def finish(v, at):
        unit = ids[5] + core * 2 * h + at + lax.broadcasted_iota(I32, (1, 256), 1)
        mask = (unit < ids[6]).astype(F32)
        return (0.5 * v * (1 + lax.erf(v * ROOT_HALF)) * mask).astype(BF16)

    def f(part):
        def block(c):
            cols, far = pl.ds(c, 256), pl.ds(c + h, 256)
            for out, mine in ((own, core), (sib, 1 - core)):
                rows = pl.ds(pl.multiple_of(mine * 64, 64), 64)
                base = pl.ds(pl.multiple_of(mine * 64 + start, 64), 64)
                v = part[base, cols] + (decode(m3_up, rows, cols) + decode(m2_dn, rows, cols)) + decode(x, rows, cols)
                out[:, cols] = finish(v, c)
                v = part[base, far] + (decode(m2_up, rows, cols) + decode(m3_dn, rows, cols)) + decode(x, rows, far)
                out[:, far] = finish(v, c + h)

        over_columns(h, 256, block)

    with_part(ids, parts, 0, f)


def earlier_kernel(ids, p0, p1, p2, p3, out, std):
    core, y, xl, z, xh = ids[0], ids[1], ids[2], ids[3], ids[4]
    for j, off in enumerate(OFFS):
        for s in range(2):
            at = lax.rem(z + off + 4, 4) * 2 + lax.rem(xh + s, 2)
            std[pl.ds(pl.multiple_of(at * 128, 128), 128), :] = (p0, p1, p2, p3)[j][s]
    for s in range(2):
        for j, off in enumerate(OFFS):
            at = lax.rem(y + off + 4, 4) * 2 + lax.rem(xl + s, 2)
            own = std[pl.ds(pl.multiple_of(at * 128 + core * 64, 64), 64), :]
            sib = std[pl.ds(pl.multiple_of(at * 128 + (1 - core) * 64, 64), 64), :]
            i = s * 4 + j
            out[:, i * 128:(i + 1) * 128] = jnp.concatenate([own, sib], axis=0).T


def grad_kernel(ids, *refs):
    own, sib, p_t, out, rhs = refs[:8], refs[8:16], refs[16], refs[17], refs[18]
    for j in range(8):
        rhs[j * 128:j * 128 + 64, :] = own[j][...]
        rhs[j * 128 + 64:j * 128 + 128, :] = sib[j][...]
    tn = out.shape[1]
    unit = ids[5] + pl.program_id(0) * tn + lax.broadcasted_iota(I32, (1, tn), 1)
    mask = (unit < ids[6]).astype(F32)
    grad = jnp.dot(p_t[...], rhs[...], preferred_element_type=F32)
    out[...] = (grad * mask).astype(BF16)


def vmem():
    return pl.BlockSpec(memory_space=pltpu.VMEM)


def shards(tokens, prev_tokens, hidden_grad, active_blocks, weight):
    slab, units = weight.shape
    half = units // 2
    row, col = lax.axis_index("row"), lax.axis_index("col")
    core = col % 2
    ids = jnp.stack([core, (col // 2) % 4, col // 8, row % 4, row // 4, row * units, active_blocks[0] * BLOCK, 0]).astype(I32)

    def call(f, outs, grid=(), specs=None, out_specs=None, scratch=(), flops=1 << 20, limit=16):
        params = pltpu.CompilerParams(vmem_limit_bytes=limit << 20)
        cost = pl.CostEstimate(flops=flops, bytes_accessed=1 << 20, transcendentals=0)
        spec = pltpu.PrefetchScalarGridSpec(num_scalar_prefetch=1, grid=grid, in_specs=specs, out_specs=out_specs, scratch_shapes=scratch)
        g = pl.pallas_call(f, grid_spec=spec, out_shape=outs, compiler_params=params, cost_estimate=cost)

        def run(*args):
            return g(ids, *args)

        return run

    def small(f, outs, *args):
        return call(f, outs, (), [vmem()] * len(args), [vmem()] * len(outs))(*args)

    def gather_row(a):
        near = jnp.stack([a, send(a, XHI)])
        return [near, send(near, ZUP), send(near, ZDN), send(near, ZTWO)]

    t_own = gather_row(tokens)
    t_sib = [send(a, SIB) for a in t_own]
    w_sib = send(weight, SIB)

    h_own = [hidden_grad, send(hidden_grad, YUP), send(hidden_grad, YDN), send(hidden_grad, YTWO)]
    h_own = h_own + [send(a, XLO) for a in h_own]
    h_sib = [send(a, SIB) for a in h_own]

    p_own = gather_row(prev_tokens)

    S = jax.ShapeDtypeStruct
    V = pltpu.VMEM
    quarter = half // 2
    hbm = pl.BlockSpec(memory_space=pltpu.HBM)
    w_half = V((slab, half), BF16)
    w_own, w_far = call(load_kernel, [w_half] * 2, (), [hbm] * 2, [vmem()] * 2, [pltpu.SemaphoreType.DMA((2,))])(weight, w_sib)

    def partials(which):
        n = len(which)
        args = [t_own[j] for j in which] + [t_sib[j] for j in which] + [w_own, w_far]
        return call(
            part_kernel, [V((256, half), F32)] * n, (), [vmem()] * len(args), [vmem()] * n,
            flops=2 * 256 * n * 2 * slab * half, limit=PART_LIMIT,
        )(*args)

    parts = partials((0,)) + partials((1, 2)) + partials((3,))
    msg, piece = V((256 + TAG, quarter), I16), V((128 + TAG, quarter), I16)
    m1_up, m1_dn = small(first_kernel, [msg] * 2, *parts)
    m1_up, m1_dn = send(m1_up, YUP), send(m1_dn, YDN)
    up1, up2, dn1, dn2 = small(second_kernel, [piece] * 4, *parts)
    m2_up1, m2_dn1 = send(up1, YUP), send(dn1, YDN)
    m2_up2, m2_dn2 = send(up2, YUP), send(dn2, YDN)
    m3_up1, m3_up2 = small(partial(relay_kernel, 1), [piece] * 2, *parts, m1_up)
    m3_dn1, m3_dn2 = small(partial(relay_kernel, -1), [piece] * 2, *parts, m1_dn)
    m3_up1, m3_dn1 = send(m3_up1, YUP), send(m3_dn1, YDN)
    m3_up2, m3_dn2 = send(m3_up2, YUP), send(m3_dn2, YDN)
    given, = small(give_kernel, [V((128 + TAG, half), I16)], *parts, m2_up1, m2_dn1, m3_up1, m3_dn1)
    x_in = send(given, XLO)
    act = V((64, half), BF16)
    act_own, act_give = small(keep_kernel, [act] * 2, *parts, m2_up2, m2_dn2, m3_up2, m3_dn2, x_in)
    act_sib = send(act_give, SIB)
    activation = jnp.where(core == 0, jnp.concatenate([act_own, act_sib], 1), jnp.concatenate([act_sib, act_own], 1))

    p_t, = call(earlier_kernel, [V((slab, 1024), BF16)], (), [vmem()] * 4, [vmem()], [V((1024, slab), BF16)])(*p_own)
    tg = 1024
    weight_grad = call(
        grad_kernel, S((slab, units), BF16), (units // tg,),
        [pl.BlockSpec((64, tg), lambda i, s: (0, i))] * 16 + [vmem()],
        pl.BlockSpec((slab, tg), lambda i, s: (0, i)), [V((1024, tg), BF16)],
        flops=2 * 1024 * slab * units, limit=24,
    )(*h_own, *h_sib, p_t)
    return (activation, weight_grad)


def solution(mesh):
    return jax.shard_map(
        shards,
        mesh=mesh,
        in_specs=(P("row", "col"), P("row", "col"), P("col", "row"), P(), P("col", "row")),
        out_specs=(P("col", "row"), P("col", "row")),
        check_vma=False,
    )
```

```python
from functools import partial

import jax
import jax.numpy as jnp
from jax import lax
from jax.experimental import pallas as pl
from jax.experimental.pallas import tpu as pltpu
from jax.sharding import PartitionSpec as P


BLOCK = 3072
ROUND = 1.5 * 2.0 ** 23
F32, BF16, I16, I32 = jnp.float32, jnp.bfloat16, jnp.int16, jnp.int32


def perm(f):
    out = []
    for i in range(128):
        r, c = divmod(i, 16)
        xh, z, xl, y, k = f(r // 4, r % 4, c // 8, (c // 2) % 4, c % 2)
        out.append((i, (xh * 4 + z % 4) * 16 + xl * 8 + (y % 4) * 2 + k))
    return out


SIB = perm(lambda h, z, x, y, k: (h, z, x, y, 1 - k))
XLO = perm(lambda h, z, x, y, k: (h, z, 1 - x, y, k))
XLO_SIB = perm(lambda h, z, x, y, k: (h, z, 1 - x, y, 1 - k))
XHI = perm(lambda h, z, x, y, k: (1 - h, z, x, y, k))
YUP = perm(lambda h, z, x, y, k: (h, z, x, y + 1, k))
YDN = perm(lambda h, z, x, y, k: (h, z, x, y - 1, k))
YTWO = perm(lambda h, z, x, y, k: (h, z, x, y + 2, k))
ZUP = perm(lambda h, z, x, y, k: (h, z + 1, x, y, k))
ZDN = perm(lambda h, z, x, y, k: (h, z - 1, x, y, k))
ZTWO = perm(lambda h, z, x, y, k: (h, z + 2, x, y, k))


def send(a, p):
    return lax.ppermute(a, ("row", "col"), p)


OFFS = (0, -1, 1, 2)
TAG = 8
PART_LIMIT = 12
ROOT_HALF = 0.5 ** 0.5


def encode(v, ref, cols, base=0):
    rows = v.shape[0]
    top = jnp.maximum(jnp.max(jnp.abs(v), axis=0, keepdims=True), 2.0 ** -100)
    e = jnp.floor(jnp.log2(top * (1 + 2.0 ** -10))) + 1
    mant = jnp.ceil(top * jnp.exp2(15 - e))
    scale = mant * jnp.exp2(e - 15) * (1 / 32767)
    q = v * (1 / scale) + ROUND - ROUND
    ref[base:base + rows, cols] = q.astype(I32).astype(I16)
    sub = lax.broadcasted_iota(I32, (TAG, v.shape[1]), 0)
    ref[base + rows:base + rows + TAG, cols] = jnp.where(sub < TAG // 2, mant, e).astype(I32).astype(I16)


def decode(ref, rows, cols):
    n = ref.shape[0] - TAG
    tag = ref[n:, cols].astype(I32).astype(F32)
    scale = tag[0:1] * jnp.exp2(tag[TAG // 2:TAG // 2 + 1] - 15) * (1 / 32767)
    return ref[rows, cols].astype(I32).astype(F32) * scale


def over_columns(n, width, body):
    def step(i, c):
        body(pl.multiple_of(i * width, width))
        return c

    lax.fori_loop(0, n // width, step, 0)


def load_kernel(ids, w, out, sem):
    half = out.shape[1]
    copy = pltpu.make_async_copy(w.at[:, pl.ds(pl.multiple_of(ids[0] * half, half), half)], out, sem.at[0])
    copy.start()
    copy.wait()


def part_kernel(ids, *refs):
    n = (len(refs) - 2) // 3
    own, sib, (w_own, w_sib), outs = refs[:n], refs[n:2 * n], refs[2 * n:2 * n + 2], refs[2 * n + 2:]
    slab, half = w_own.shape
    lhs = jnp.concatenate(
        [jnp.concatenate([a[...].reshape(256, slab), b[...].reshape(256, slab)], axis=1) for a, b in zip(own, sib)], axis=0
    )

    def block(c):
        cols = pl.ds(c, 512)
        part = jnp.dot(lhs, jnp.concatenate([w_own[:, cols], w_sib[:, cols]], axis=0), preferred_element_type=F32)
        for j, out in enumerate(outs):
            out[:, cols] = part[j * 256:(j + 1) * 256]

    for c in range(0, half, 512):
        block(c)


def with_part(ids, parts, off, f):
    k = lax.rem(ids[1] - ids[3] + off + 8, 4)
    for part, j in zip(parts, (0, 3, 1, 2)):
        pl.when(k == j)(lambda part=part: f(part))


def side(ids, s):
    return pl.ds(pl.multiple_of(lax.rem(ids[2] + ids[4] + 1 + s, 2) * 128, 128), 128)


def first_kernel(ids, *refs):
    parts, (m_up, m_dn) = refs[:4], refs[4:]
    h = m_up.shape[1]

    def f(part):
        def block(c):
            cols, far = pl.ds(c, 256), pl.ds(c + h, 256)
            for out, at in ((m_up, cols), (m_dn, far)):
                encode(jnp.concatenate([part[side(ids, 0), at], part[side(ids, 1), at]], axis=0), out, cols)

        over_columns(h, 256, block)

    with_part(ids, parts, 2, f)


def second_kernel(ids, *refs):
    parts, (up, dn) = refs[:4], refs[4:]
    h = up.shape[1]

    def go(part, out, base):
        def block(c):
            encode(part[side(ids, 0), pl.ds(c + base, 256)], out, pl.ds(c, 256))

        over_columns(h, 256, block)

    with_part(ids, parts, 1, lambda part: go(part, up, h))
    with_part(ids, parts, -1, lambda part: go(part, dn, 0))


def relay_kernel(off, ids, *refs):
    parts, m, first, second = refs[:4], refs[4], refs[5], refs[6]
    h = m.shape[1]
    base, rest = (0, h) if off == 1 else (h, 0)

    def f(part):
        def block(c):
            cols, at, other = pl.ds(c, 256), pl.ds(c + base, 256), pl.ds(c + rest, 256)
            encode(part[side(ids, 0), at] + decode(m, slice(0, 128), cols), first, cols)
            encode(part[side(ids, 1), at] + decode(m, slice(128, 256), cols), second, at)
            encode(part[side(ids, 1), other], second, other)

        over_columns(h, 256, block)

    with_part(ids, parts, off, f)


def give_kernel(ids, *refs):
    parts, (m2_up, m2_dn, m3_up, m3_dn, same, cross) = refs[:4], refs[4:]
    h = m2_up.shape[1]
    core = ids[0]
    start = lax.rem(ids[2] + ids[4] + 1, 2) * 128

    def f(part):
        def block(c):
            cols, far = pl.ds(c, 256), pl.ds(c + h, 256)
            for out, mine in ((same, core), (cross, 1 - core)):
                rows = pl.ds(pl.multiple_of(mine * 64, 64), 64)
                base = pl.ds(pl.multiple_of(mine * 64 + start, 64), 64)
                encode(part[base, cols] + (decode(m3_up, rows, cols) + decode(m2_dn, rows, cols)), out, cols)
                encode(part[base, far] + (decode(m2_up, rows, cols) + decode(m3_dn, rows, cols)), out, far)

        over_columns(h, 256, block)

    with_part(ids, parts, 0, f)


def sum_kernel(ids, *refs):
    parts, (up, dn, own, sib) = refs[:4], refs[4:]
    start = lax.rem(ids[2] + ids[4], 2) * 128

    def f(part):
        def block(c):
            cols = pl.ds(c, 256)
            for out, mine in ((own, ids[0]), (sib, 1 - ids[0])):
                rows = pl.ds(pl.multiple_of(mine * 64, 64), 64)
                base = pl.ds(pl.multiple_of(mine * 64 + start, 64), 64)
                out[:, cols] = part[base, cols] + (decode(up, rows, cols) + decode(dn, rows, cols))

        over_columns(own.shape[1], 256, block)

    with_part(ids, parts, 0, f)


def keep_kernel(ids, own, sib, x_own, x_sib, out):
    half = own.shape[1]
    for v, x, k in ((own, x_own, ids[0]), (sib, x_sib, 1 - ids[0])):
        def block(c):
            cols = pl.ds(c, 256)
            at = k * half + c
            hidden = v[:, cols] + decode(x, slice(0, 64), cols)
            unit = ids[5] + at + lax.broadcasted_iota(I32, (1, 256), 1)
            mask = (unit < ids[6]).astype(F32)
            act = 0.5 * hidden * (1 + lax.erf(hidden * ROOT_HALF)) * mask
            out[:, pl.ds(pl.multiple_of(at, 256), 256)] = act.astype(BF16)

        over_columns(half, 256, block)


def earlier_kernel(ids, p0, p1, p2, p3, out, std):
    core, y, xl, z, xh = ids[0], ids[1], ids[2], ids[3], ids[4]
    for j, off in enumerate(OFFS):
        for s in range(2):
            at = lax.rem(z + off + 4, 4) * 2 + lax.rem(xh + s, 2)
            std[pl.ds(pl.multiple_of(at * 128, 128), 128), :] = (p0, p1, p2, p3)[j][s]
    for s in range(2):
        for j, off in enumerate(OFFS):
            at = lax.rem(y + off + 4, 4) * 2 + lax.rem(xl + s, 2)
            own = std[pl.ds(pl.multiple_of(at * 128 + core * 64, 64), 64), :]
            sib = std[pl.ds(pl.multiple_of(at * 128 + (1 - core) * 64, 64), 64), :]
            i = s * 4 + j
            out[:, i * 128:(i + 1) * 128] = jnp.concatenate([own, sib], axis=0).T


def grad_kernel(base, ids, *refs):
    near, p_t, out, rhs = refs[:16], refs[16], refs[-2], refs[-1]
    own = near[:3] + near[12:13] + near[3:6] + near[13:14]
    sib = near[6:9] + near[14:15] + near[9:12] + near[15:16]
    for j in range(8):
        rhs[j * 128:j * 128 + 64, :] = own[j][...]
        rhs[j * 128 + 64:j * 128 + 128, :] = sib[j][...]
    tn = out.shape[1]
    unit = ids[5] + (pl.program_id(0) + base) * tn + lax.broadcasted_iota(I32, (1, tn), 1)
    mask = (unit < ids[6]).astype(F32)
    grad = jnp.dot(p_t[...], rhs[...], preferred_element_type=F32)
    out[...] = (grad * mask).astype(BF16)


def vmem():
    return pl.BlockSpec(memory_space=pltpu.VMEM)


def shards(tokens, prev_tokens, hidden_grad, active_blocks, weight):
    slab, units = weight.shape
    half = units // 2
    row, col = lax.axis_index("row"), lax.axis_index("col")
    core = col % 2
    ids = jnp.stack([core, (col // 2) % 4, col // 8, row % 4, row // 4, row * units, active_blocks[0] * BLOCK, 0]).astype(I32)

    def call(f, outs, grid=(), specs=None, out_specs=None, scratch=(), flops=1 << 20, limit=8):
        params = pltpu.CompilerParams(vmem_limit_bytes=limit << 20)
        cost = pl.CostEstimate(flops=flops, bytes_accessed=1 << 20, transcendentals=0)
        spec = pltpu.PrefetchScalarGridSpec(num_scalar_prefetch=1, grid=grid, in_specs=specs, out_specs=out_specs, scratch_shapes=scratch)
        g = pl.pallas_call(f, grid_spec=spec, out_shape=outs, compiler_params=params, cost_estimate=cost)

        def run(*args):
            return g(ids, *args)

        return run

    def small(f, outs, *args):
        return call(f, outs, (), [vmem()] * len(args), [vmem()] * len(outs))(*args)

    def gather_row(a):
        near = jnp.stack([a, send(a, XHI)])
        return [near, send(near, ZUP), send(near, ZDN), send(near, ZTWO)]

    t_own = gather_row(tokens)
    t_sib = [send(a, SIB) for a in t_own]
    w_sib = send(weight, SIB)

    h_near = [hidden_grad, send(hidden_grad, YUP), send(hidden_grad, YDN)]
    h_left = send(h_near[1][:, :half], YUP)
    h_right = send(h_near[2][:, half:], YDN)
    far = lambda a: send(a, XLO)
    h_near = h_near + [far(a) for a in h_near]
    h_left, h_right = [h_left, far(h_left)], [h_right, far(h_right)]
    s_near = [send(a, SIB) for a in h_near]
    s_left = [send(a, SIB) for a in h_left]
    s_right = [send(a, SIB) for a in h_right]

    p_own = gather_row(prev_tokens)

    S = jax.ShapeDtypeStruct
    V = pltpu.VMEM
    quarter = half // 2
    hbm = pl.BlockSpec(memory_space=pltpu.HBM)
    w_half = V((slab, half), BF16)

    def load(w, limit):
        return call(load_kernel, [w_half], (), [hbm], [vmem()], [pltpu.SemaphoreType.DMA((1,))], limit=limit)(w)[0]

    w_own, w_far = load(weight, 50), load(w_sib, 46)

    def partials(which):
        n = len(which)
        args = [t_own[j] for j in which] + [t_sib[j] for j in which] + [w_own, w_far]
        return call(
            part_kernel, [V((256, half), F32)] * n, (), [vmem()] * len(args), [vmem()] * n,
            flops=2 * 256 * n * 2 * slab * half, limit=PART_LIMIT,
        )(*args)

    parts = partials((0,)) + partials((1, 2)) + partials((3,))
    msg, piece = V((256 + TAG, quarter), I16), V((128 + TAG, quarter), I16)
    m1_up, m1_dn = small(first_kernel, [msg] * 2, *parts)
    m1_up, m1_dn = send(m1_up, YUP), send(m1_dn, YDN)
    m2_up, m2_dn = small(second_kernel, [piece] * 2, *parts)
    m2_up, m2_dn = send(m2_up, YUP), send(m2_dn, YDN)
    wide = V((128 + TAG, half), I16)
    m3_up, m4_up = small(partial(relay_kernel, 1), [piece, wide], *parts, m1_up)
    m3_dn, m4_dn = small(partial(relay_kernel, -1), [piece, wide], *parts, m1_dn)
    m3_up, m3_dn = send(m3_up, YUP), send(m3_dn, YDN)
    m4_up, m4_dn = send(m4_up, YUP), send(m4_dn, YDN)
    same, cross = small(give_kernel, [V((64 + TAG, half), I16)] * 2, *parts, m2_up, m2_dn, m3_up, m3_dn)
    x_own, x_sib = send(same, XLO), send(cross, XLO_SIB)
    kept, other = small(sum_kernel, [V((64, half), F32)] * 2, *parts, m4_up, m4_dn)
    other = send(other, SIB)
    activation, = small(keep_kernel, [S((64, units), BF16)], kept, other, x_own, x_sib)

    p_t, = call(earlier_kernel, [V((slab, 1024), BF16)], (), [vmem()] * 4, [vmem()], [V((1024, slab), BF16)])(*p_own)
    tg = 1024
    steps = units // tg // 2

    def grad(base, far, *before):
        return pl.pallas_call(
            partial(grad_kernel, base), out_shape=S((slab, units), BF16),
            grid_spec=pltpu.PrefetchScalarGridSpec(
                num_scalar_prefetch=1, grid=(steps,),
                in_specs=[pl.BlockSpec((64, tg), lambda i, s: (0, i + base))] * 12 + [pl.BlockSpec((64, tg), lambda i, s: (0, i))] * 4
                + [vmem()] + [pl.BlockSpec(memory_space=pl.ANY)] * len(before),
                out_specs=pl.BlockSpec((slab, tg), lambda i, s: (0, i + base)), scratch_shapes=[V((1024, tg), BF16)],
            ),
            compiler_params=pltpu.CompilerParams(vmem_limit_bytes=24 << 20),
            cost_estimate=pl.CostEstimate(flops=1024 * slab * units, bytes_accessed=1 << 20, transcendentals=0),
            input_output_aliases={18: 0} if before else {},
        )(ids, *h_near, *s_near, *far, p_t, *before)

    weight_grad = grad(steps, h_right + s_right, grad(0, h_left + s_left))
    return (activation, weight_grad)


def solution(mesh):
    return jax.shard_map(
        shards,
        mesh=mesh,
        in_specs=(P("row", "col"), P("row", "col"), P("col", "row"), P(), P("col", "row")),
        out_specs=(P("col", "row"), P("col", "row")),
        check_vma=False,
    )
```

```python
from functools import partial

import jax
import jax.numpy as jnp
from jax import lax
from jax.experimental import pallas as pl
from jax.experimental.pallas import tpu as pltpu
from jax.sharding import PartitionSpec as P


BLOCK = 3072
ROUND = 1.5 * 2.0 ** 23
F32, BF16, I16, I32 = jnp.float32, jnp.bfloat16, jnp.int16, jnp.int32


def perm(f):
    out = []
    for i in range(128):
        r, c = divmod(i, 16)
        xh, z, xl, y, k = f(r // 4, r % 4, c // 8, (c // 2) % 4, c % 2)
        out.append((i, (xh * 4 + z % 4) * 16 + xl * 8 + (y % 4) * 2 + k))
    return out


SIB = perm(lambda h, z, x, y, k: (h, z, x, y, 1 - k))
XLO = perm(lambda h, z, x, y, k: (h, z, 1 - x, y, k))
XLO_SIB = perm(lambda h, z, x, y, k: (h, z, 1 - x, y, 1 - k))
XHI = perm(lambda h, z, x, y, k: (1 - h, z, x, y, k))
YUP = perm(lambda h, z, x, y, k: (h, z, x, y + 1, k))
YDN = perm(lambda h, z, x, y, k: (h, z, x, y - 1, k))
YTWO = perm(lambda h, z, x, y, k: (h, z, x, y + 2, k))
ZUP = perm(lambda h, z, x, y, k: (h, z + 1, x, y, k))
ZDN = perm(lambda h, z, x, y, k: (h, z - 1, x, y, k))
ZTWO = perm(lambda h, z, x, y, k: (h, z + 2, x, y, k))


def send(a, p):
    return lax.ppermute(a, ("row", "col"), p)


OFFS = (0, -1, 1, 2)
TAG = 8
PART_LIMIT = 12
ROOT_HALF = 0.5 ** 0.5


def encode(v, ref, cols, base=0):
    rows = v.shape[0]
    top = jnp.maximum(jnp.max(jnp.abs(v), axis=0, keepdims=True), 2.0 ** -100)
    e = jnp.floor(jnp.log2(top * (1 + 2.0 ** -10))) + 1
    mant = jnp.ceil(top * jnp.exp2(15 - e))
    scale = mant * jnp.exp2(e - 15) * (1 / 32767)
    q = v * (1 / scale) + ROUND - ROUND
    ref[base:base + rows, cols] = q.astype(I32).astype(I16)
    sub = lax.broadcasted_iota(I32, (TAG, v.shape[1]), 0)
    ref[base + rows:base + rows + TAG, cols] = jnp.where(sub < TAG // 2, mant, e).astype(I32).astype(I16)


def decode(ref, rows, cols):
    n = ref.shape[0] - TAG
    tag = ref[n:, cols].astype(I32).astype(F32)
    scale = tag[0:1] * jnp.exp2(tag[TAG // 2:TAG // 2 + 1] - 15) * (1 / 32767)
    return ref[rows, cols].astype(I32).astype(F32) * scale


def over_columns(n, width, body):
    def step(i, c):
        body(pl.multiple_of(i * width, width))
        return c

    lax.fori_loop(0, n // width, step, 0)


def load_kernel(ids, w, out, sem):
    half = out.shape[1]
    copy = pltpu.make_async_copy(w.at[:, pl.ds(pl.multiple_of(ids[0] * half, half), half)], out, sem.at[0])
    copy.start()
    copy.wait()


def part_kernel(ids, *refs):
    n = (len(refs) - 2) // 3
    own, sib, (w_own, w_sib), outs = refs[:n], refs[n:2 * n], refs[2 * n:2 * n + 2], refs[2 * n + 2:]
    slab, half = w_own.shape
    lhs = jnp.concatenate(
        [jnp.concatenate([a[...].reshape(256, slab), b[...].reshape(256, slab)], axis=1) for a, b in zip(own, sib)], axis=0
    )

    def block(c):
        cols = pl.ds(c, 512)
        part = jnp.dot(lhs, jnp.concatenate([w_own[:, cols], w_sib[:, cols]], axis=0), preferred_element_type=F32)
        for j, out in enumerate(outs):
            out[:, cols] = part[j * 256:(j + 1) * 256]

    for c in range(0, half, 512):
        block(c)


def with_part(ids, parts, off, f):
    k = lax.rem(ids[1] - ids[3] + off + 8, 4)
    for part, j in zip(parts, (0, 3, 1, 2)):
        pl.when(k == j)(lambda part=part: f(part))


def side(ids, s):
    return pl.ds(pl.multiple_of(lax.rem(ids[2] + ids[4] + 1 + s, 2) * 128, 128), 128)


def first_kernel(ids, *refs):
    parts, (m_up, m_dn) = refs[:4], refs[4:]
    h = m_up.shape[1]

    def f(part):
        def block(c):
            cols, far = pl.ds(c, 256), pl.ds(c + h, 256)
            for out, at in ((m_up, cols), (m_dn, far)):
                encode(jnp.concatenate([part[side(ids, 0), at], part[side(ids, 1), at]], axis=0), out, cols)

        over_columns(h, 256, block)

    with_part(ids, parts, 2, f)


def second_kernel(ids, *refs):
    parts, (up, dn) = refs[:4], refs[4:]
    h = up.shape[1]

    def go(part, out, base):
        def block(c):
            encode(part[side(ids, 0), pl.ds(c + base, 256)], out, pl.ds(c, 256))

        over_columns(h, 256, block)

    with_part(ids, parts, 1, lambda part: go(part, up, h))
    with_part(ids, parts, -1, lambda part: go(part, dn, 0))


def relay_kernel(off, ids, *refs):
    parts, m, first, second = refs[:4], refs[4], refs[5], refs[6]
    h = m.shape[1]
    base, rest = (0, h) if off == 1 else (h, 0)

    def f(part):
        def block(c):
            cols, at, other = pl.ds(c, 256), pl.ds(c + base, 256), pl.ds(c + rest, 256)
            encode(part[side(ids, 0), at] + decode(m, slice(0, 128), cols), first, cols)
            encode(part[side(ids, 1), at] + decode(m, slice(128, 256), cols), second, at)
            encode(part[side(ids, 1), other], second, other)

        over_columns(h, 256, block)

    with_part(ids, parts, off, f)


def give_kernel(ids, *refs):
    parts, (m2_up, m2_dn, m3_up, m3_dn, same, cross) = refs[:4], refs[4:]
    h = m2_up.shape[1]
    core = ids[0]
    start = lax.rem(ids[2] + ids[4] + 1, 2) * 128

    def f(part):
        def block(c):
            cols, far = pl.ds(c, 256), pl.ds(c + h, 256)
            for out, mine in ((same, core), (cross, 1 - core)):
                rows = pl.ds(pl.multiple_of(mine * 64, 64), 64)
                base = pl.ds(pl.multiple_of(mine * 64 + start, 64), 64)
                encode(part[base, cols] + (decode(m3_up, rows, cols) + decode(m2_dn, rows, cols)), out, cols)
                encode(part[base, far] + (decode(m2_up, rows, cols) + decode(m3_dn, rows, cols)), out, far)

        over_columns(h, 256, block)

    with_part(ids, parts, 0, f)


def sum_kernel(ids, *refs):
    parts, (up, dn, own, sib) = refs[:4], refs[4:]
    start = lax.rem(ids[2] + ids[4], 2) * 128

    def f(part):
        def block(c):
            cols = pl.ds(c, 256)
            for out, mine in ((own, ids[0]), (sib, 1 - ids[0])):
                rows = pl.ds(pl.multiple_of(mine * 64, 64), 64)
                base = pl.ds(pl.multiple_of(mine * 64 + start, 64), 64)
                out[:, cols] = part[base, cols] + (decode(up, rows, cols) + decode(dn, rows, cols))

        over_columns(own.shape[1], 256, block)

    with_part(ids, parts, 0, f)


def keep_kernel(ids, own, sib, x_own, x_sib, out):
    half = own.shape[1]
    for v, x, k in ((own, x_own, ids[0]), (sib, x_sib, 1 - ids[0])):
        def block(c):
            cols = pl.ds(c, 256)
            at = k * half + c
            hidden = v[:, cols] + decode(x, slice(0, 64), cols)
            unit = ids[5] + at + lax.broadcasted_iota(I32, (1, 256), 1)
            mask = (unit < ids[6]).astype(F32)
            act = 0.5 * hidden * (1 + lax.erf(hidden * ROOT_HALF)) * mask
            out[:, pl.ds(pl.multiple_of(at, 256), 256)] = act.astype(BF16)

        over_columns(half, 256, block)


def earlier_kernel(ids, p0, p1, p2, p3, out, std):
    core, y, xl, z, xh = ids[0], ids[1], ids[2], ids[3], ids[4]
    for j, off in enumerate(OFFS):
        for s in range(2):
            at = lax.rem(z + off + 4, 4) * 2 + lax.rem(xh + s, 2)
            std[pl.ds(pl.multiple_of(at * 128, 128), 128), :] = (p0, p1, p2, p3)[j][s]
    for s in range(2):
        for j, off in enumerate(OFFS):
            at = lax.rem(y + off + 4, 4) * 2 + lax.rem(xl + s, 2)
            own = std[pl.ds(pl.multiple_of(at * 128 + core * 64, 64), 64), :]
            sib = std[pl.ds(pl.multiple_of(at * 128 + (1 - core) * 64, 64), 64), :]
            i = s * 4 + j
            out[:, i * 128:(i + 1) * 128] = jnp.concatenate([own, sib], axis=0).T


def grad_kernel(base, ids, *refs):
    near, p_t, out, rhs = refs[:16], refs[16], refs[-2], refs[-1]
    own = near[:3] + near[12:13] + near[3:6] + near[13:14]
    sib = near[6:9] + near[14:15] + near[9:12] + near[15:16]
    for j in range(8):
        rhs[j * 128:j * 128 + 64, :] = own[j][...]
        rhs[j * 128 + 64:j * 128 + 128, :] = sib[j][...]
    tn = out.shape[1]
    unit = ids[5] + (pl.program_id(0) + base) * tn + lax.broadcasted_iota(I32, (1, tn), 1)
    mask = (unit < ids[6]).astype(F32)
    grad = jnp.dot(p_t[...], rhs[...], preferred_element_type=F32)
    out[...] = (grad * mask).astype(BF16)


def vmem():
    return pl.BlockSpec(memory_space=pltpu.VMEM)


def shards(tokens, prev_tokens, hidden_grad, active_blocks, weight):
    slab, units = weight.shape
    half = units // 2
    row, col = lax.axis_index("row"), lax.axis_index("col")
    core = col % 2
    ids = jnp.stack([core, (col // 2) % 4, col // 8, row % 4, row // 4, row * units, active_blocks[0] * BLOCK, 0]).astype(I32)

    def call(f, outs, grid=(), specs=None, out_specs=None, scratch=(), flops=1 << 20, limit=8):
        params = pltpu.CompilerParams(vmem_limit_bytes=limit << 20)
        cost = pl.CostEstimate(flops=flops, bytes_accessed=1 << 20, transcendentals=0)
        spec = pltpu.PrefetchScalarGridSpec(num_scalar_prefetch=1, grid=grid, in_specs=specs, out_specs=out_specs, scratch_shapes=scratch)
        g = pl.pallas_call(f, grid_spec=spec, out_shape=outs, compiler_params=params, cost_estimate=cost)

        def run(*args):
            return g(ids, *args)

        return run

    def small(f, outs, *args):
        return call(f, outs, (), [vmem()] * len(args), [vmem()] * len(outs))(*args)

    def gather_row(a):
        near = jnp.stack([a, send(a, XHI)])
        return [near, send(near, ZUP), send(near, ZDN), send(near, ZTWO)]

    t_own = gather_row(tokens)
    t_sib = [send(a, SIB) for a in t_own]
    w_sib = send(weight, SIB)

    h_near = [hidden_grad, send(hidden_grad, YUP), send(hidden_grad, YDN)]
    h_left = send(h_near[1][:, :half], YUP)
    h_right = send(h_near[2][:, half:], YDN)
    far = lambda a: send(a, XLO)
    h_near = h_near + [far(a) for a in h_near]
    h_left, h_right = [h_left, far(h_left)], [h_right, far(h_right)]
    s_near = [send(a, SIB) for a in h_near]
    s_left = [send(a, SIB) for a in h_left]
    s_right = [send(a, SIB) for a in h_right]

    p_own = gather_row(prev_tokens)

    S = jax.ShapeDtypeStruct
    V = pltpu.VMEM
    quarter = half // 2
    hbm = pl.BlockSpec(memory_space=pltpu.HBM)
    w_half = V((slab, half), BF16)

    def load(w, limit):
        return call(load_kernel, [w_half], (), [hbm], [vmem()], [pltpu.SemaphoreType.DMA((1,))], limit=limit)(w)[0]

    w_own, w_far = load(weight, 50), load(w_sib, 46)

    def partials(which):
        n = len(which)
        args = [t_own[j] for j in which] + [t_sib[j] for j in which] + [w_own, w_far]
        return call(
            part_kernel, [V((256, half), F32)] * n, (), [vmem()] * len(args), [vmem()] * n,
            flops=2 * 256 * n * 2 * slab * half, limit=PART_LIMIT,
        )(*args)

    parts = partials((0,)) + partials((1, 2)) + partials((3,))
    msg, piece = V((256 + TAG, quarter), I16), V((128 + TAG, quarter), I16)
    m1_up, m1_dn = small(first_kernel, [msg] * 2, *parts)
    m1_up, m1_dn = send(m1_up, YUP), send(m1_dn, YDN)
    m2_up, m2_dn = small(second_kernel, [piece] * 2, *parts)
    m2_up, m2_dn = send(m2_up, YUP), send(m2_dn, YDN)
    wide = V((128 + TAG, half), I16)
    m3_up, m4_up = small(partial(relay_kernel, 1), [piece, wide], *parts, m1_up)
    m3_dn, m4_dn = small(partial(relay_kernel, -1), [piece, wide], *parts, m1_dn)
    m3_up, m3_dn = send(m3_up, YUP), send(m3_dn, YDN)
    m4_up, m4_dn = send(m4_up, YUP), send(m4_dn, YDN)
    same, cross = small(give_kernel, [V((64 + TAG, half), I16)] * 2, *parts, m2_up, m2_dn, m3_up, m3_dn)
    x_own, x_sib = send(same, XLO), send(cross, XLO_SIB)
    kept, other = small(sum_kernel, [V((64, half), F32)] * 2, *parts, m4_up, m4_dn)
    other = send(other, SIB)
    activation, = small(keep_kernel, [S((64, units), BF16)], kept, other, x_own, x_sib)

    p_t, = call(earlier_kernel, [V((slab, 1024), BF16)], (), [vmem()] * 4, [vmem()], [V((1024, slab), BF16)])(*p_own)
    tg = 1024
    steps = units // tg // 2

    def grad(base, count, far, *before):
        return pl.pallas_call(
            partial(grad_kernel, base), out_shape=S((slab, units), BF16),
            grid_spec=pltpu.PrefetchScalarGridSpec(
                num_scalar_prefetch=1, grid=(count,),
                in_specs=[pl.BlockSpec((64, tg), lambda i, s: (0, i + base))] * 12 + [pl.BlockSpec((64, tg), lambda i, s: (0, i + base % steps))] * 4
                + [vmem()] + [pl.BlockSpec(memory_space=pl.ANY)] * len(before),
                out_specs=pl.BlockSpec((slab, tg), lambda i, s: (0, i + base)), scratch_shapes=[V((1024, tg), BF16)],
            ),
            compiler_params=pltpu.CompilerParams(vmem_limit_bytes=24 << 20),
            cost_estimate=pl.CostEstimate(flops=2 * 1024 * slab * tg * count, bytes_accessed=1 << 20, transcendentals=0),
            input_output_aliases={18: 0} if before else {},
        )(ids, *h_near, *s_near, *far, p_t, *before)

    weight_grad = grad(0, steps, h_left + s_left)
    weight_grad = grad(steps, steps - 1, h_right + s_right, weight_grad)
    weight_grad = grad(2 * steps - 1, 1, h_right + s_right, weight_grad)
    return (activation, weight_grad)


def solution(mesh):
    return jax.shard_map(
        shards,
        mesh=mesh,
        in_specs=(P("row", "col"), P("row", "col"), P("col", "row"), P(), P("col", "row")),
        out_specs=(P("col", "row"), P("col", "row")),
        check_vma=False,
    )
```
